32 devices in a mesh: pts: 16 (over z, y, x), comp: 2 (over core).
Axes of the slice: x: 2, y: 2, z: 4, core: 2. Of those that a mesh axis runs over, the one named last changes fastest.
Arguments:
- data: bfloat16 [2048, 4096], P('pts', 'comp')
- base_precision: float32 [4096], P('comp'), may hold values from 0.02 to 0.2
- offsets: float32 [4096], P('comp'), may hold values from -2 to 2
- tile_values: bfloat16 [2, 48, 128, 128], P('comp', 'pts'), may hold values from -0.3125 to 0.3125
- tile_rows: int32 [2, 48], P('comp'), may hold values from 0 to 15, as said below
- tile_cols: int32 [2, 48], P('comp'), may hold values from 0 to 31
- tile_counts: int32 [2], P('comp'), may hold values from 12 to 48, as said below
Outputs:
- log_resp: float32 [2048, 4096], P('pts', 'comp')
- point_loglik: float32 [2048], P(('pts', 'comp'))
- mean_loglik: float32 [], replicated
The draws below stay inside these ranges and needn't reach their ends.
Inputs may be any that keep to these rules, and one draw needn't show every extreme that they name: Within a group, the (tile_rows, tile_cols) pairs of all 48 slots are distinct. The live slots of group g are slots 0 to tile_counts[g] - 1; some group has all 48 slots live.
All inputs are finite; a program needn't handle non-finite values.
Results may differ from the reference program's by a relative error of at most 0.0003.
Values may be sent and summed in bfloat16 or wider, within the bound.
No kernel may reach another device: no remote copies, remote signals or barrier semaphores. Data moves between devices by JAX's collectives and lax.ppermute only.
A program may use at most 64 MiB of HBM per device.

```python
import math
import jax
import jax.numpy as jnp
from jax import lax

F = 4096
COMP_DEV = 2048
BLOCK = 128
TILES = 48
POINTS = 2048
COMPONENTS = 4096
N_COMP = 2


def draw_data(key, part):
    position = jnp.arange(POINTS, dtype=jnp.float32) / POINTS
    rising = 1.0 + 0.8 * position
    stretch = max(1.0, (400.0 / (0.07 * F)) ** 0.5)
    chosen = jax.random.randint(jax.random.fold_in(key, 5), (POINTS,), 0, 8) == 0
    loud = jnp.where(chosen, stretch, 1.0).astype(jnp.float32)
    values = jax.random.normal(key, (POINTS, F), jnp.float32)
    return (values * (rising * loud)[:, None]).astype(jnp.bfloat16)


def tile_positions(key):
    keys = jax.random.split(jax.random.fold_in(key, 7), N_COMP)
    cells = COMP_DEV // BLOCK * (F // BLOCK)
    perms = jax.vmap(lambda single: jax.random.permutation(single, cells))(keys)
    return perms[:, :TILES].astype(jnp.int32)


def draw_tile_rows(key, part):
    return tile_positions(key) // (F // BLOCK)


def draw_tile_cols(key, part):
    return tile_positions(key) % (F // BLOCK)


def draw_tile_counts(key, part):
    counts = jax.random.randint(jax.random.fold_in(key, 11), (N_COMP,), TILES // 4, TILES + 1)
    fullest = jax.random.randint(jax.random.fold_in(key, 12), (), 0, N_COMP)
    counts = counts.at[fullest].set(TILES)
    return counts.astype(jnp.int32)


def block_scale(stream_key, shape, cuts, smallest, high):
    def one(dim, parts):
        draws = jax.random.uniform(jax.random.fold_in(jax.random.fold_in(stream_key, 6), dim), (parts,), jnp.float32, smallest / len(cuts), high / len(cuts))
        return jnp.repeat(jnp.exp(draws), shape[dim] // parts).reshape((-1,) + (1,) * (len(shape) - dim - 1))

    level = one(*cuts[0])
    for cut in cuts[1:]:
        level = level * one(*cut)
    return level


def noise(own_key, shape, scale, bound, cuts=(), held_as=jnp.bfloat16):
    drawn = scale * jax.random.normal(own_key, shape, jnp.float32)
    if cuts:
        drawn = drawn * block_scale(own_key, shape, cuts, -0.22, 0.18)
    return jnp.clip(drawn, -bound, bound).astype(held_as)


def setup_inputs(seed: int = 0) -> dict:
    seeds = jax.random.split(jax.random.key(seed), 8)
    return {
        "data": draw_data(jax.random.fold_in(seeds[7], 71), 0),
        "base_precision": jnp.clip(jnp.exp(math.log(0.2) - 2.3025851 * jax.random.uniform(seeds[1], (F,), jnp.float32) ** block_scale(seeds[1], (F,), ((0, 2),), -0.2, 0.2)), 0.02, 0.2),
        "offsets": jnp.clip(jax.random.uniform(seeds[2], (COMPONENTS,), jnp.float32, -2.0, 2.0) * block_scale(seeds[2], (COMPONENTS,), ((0, 2),), -0.4, 0.0), -2.0, 2.0),
        "tile_values": noise(seeds[3], (N_COMP, TILES, BLOCK, BLOCK), (3 * BLOCK) ** -0.5, 0.3125, ((0, 2), (1, 16))),
        "tile_rows": draw_tile_rows(jax.random.fold_in(seeds[7], 71), 0),
        "tile_cols": draw_tile_cols(jax.random.fold_in(seeds[7], 71), 0),
        "tile_counts": draw_tile_counts(jax.random.fold_in(seeds[7], 71), 0),
    }


def group_scores(data, offsets_group, values_group, rows_group, cols_group, count_group, quad):
    def step(total, slot):
        col = cols_group[slot].astype(jnp.int32)
        row = rows_group[slot].astype(jnp.int32)
        panel = lax.dynamic_slice_in_dim(data, col * BLOCK, BLOCK, 1)
        product = jnp.dot(panel, values_group[slot], preferred_element_type=jnp.float32)
        live = (slot < count_group).astype(jnp.float32)
        current = lax.dynamic_slice_in_dim(total, row * BLOCK, BLOCK, 1)
        total = lax.dynamic_update_slice_in_dim(total, current + live * product, row * BLOCK, 1)
        return total, None

    start = jnp.zeros((data.shape[0], COMP_DEV), jnp.float32)
    total, _ = lax.scan(step, start, jnp.arange(TILES, dtype=jnp.int32))
    return total + offsets_group[None, :] + quad[:, None]


def reference(data, base_precision, offsets, tile_values, tile_rows, tile_cols, tile_counts):
    squares = data.astype(jnp.float32) ** 2
    quad = -0.5 * jnp.dot(squares, base_precision, precision=lax.Precision.HIGHEST)
    grouped = offsets.reshape(N_COMP, COMP_DEV)

    def one_group(items):
        offs, values, rows, cols, count = items
        return group_scores(data, offs, values, rows, cols, count, quad)

    scores = lax.map(one_group, (grouped, tile_values, tile_rows, tile_cols, tile_counts))
    peak = jnp.max(jnp.max(scores, axis=2), axis=0)
    mass = jnp.sum(jnp.sum(jnp.exp(scores - peak[None, :, None]), axis=2), axis=0)
    lse = peak + jnp.log(mass)
    log_resp = (scores - lse[None, :, None]).transpose(1, 0, 2).reshape(data.shape[0], N_COMP * COMP_DEV)
    point_loglik = lse / (F // BLOCK)
    mean_loglik = jnp.sum(point_loglik) / data.shape[0]
    return log_resp, point_loglik, mean_loglik
```

```python
import functools

import jax
import jax.numpy as jnp
from jax import lax
from jax.experimental import pallas as pl
from jax.experimental.pallas import tpu as pltpu
from jax.sharding import PartitionSpec as P

BLOCK = 128
VMEM_LIMIT = 16 * 1024 * 1024

vmem = pl.BlockSpec(memory_space=pltpu.VMEM)
smem = pl.BlockSpec(memory_space=pltpu.SMEM)


def call(body, name, out_shape, in_specs, args, flops):
    return pl.pallas_call(
        body,
        name=name,
        out_shape=out_shape,
        in_specs=in_specs,
        out_specs=jax.tree.map(lambda _: vmem, out_shape),
        compiler_params=pltpu.CompilerParams(vmem_limit_bytes=VMEM_LIMIT),
        cost_estimate=pl.CostEstimate(flops=flops, bytes_accessed=1 << 20, transcendentals=0),
    )(*args)


def prepare(n_comp, precision_ref, *refs):
    data_refs, (blocks_ref, quad_ref) = refs[:n_comp], refs[n_comp:]
    here = lax.axis_index("comp")
    hblocks = data_refs[0].shape[1] // BLOCK
    total = jnp.zeros((data_refs[0].shape[0], BLOCK), jnp.float32)
    for shift, data_ref in enumerate(data_refs):
        owner = lax.rem(here - shift + n_comp, n_comp)
        for b in range(hblocks):
            lanes = slice(b * BLOCK, (b + 1) * BLOCK)
            block = data_ref[:, lanes]
            blocks_ref[owner * hblocks + b] = block
            if shift == 0:
                wide = block.astype(jnp.float32)
                total += wide * wide * precision_ref[:, lanes]
    quad_ref[...] = jnp.broadcast_to(-0.5 * jnp.sum(total, axis=1, keepdims=True), quad_ref.shape)


def add_tiles(masks, blocks_ref, rows_ref, cols_ref, count_ref, pieces, acc_ref):
    me = lax.axis_index("pts")
    spare = acc_ref.shape[0] - 1
    for mask, piece in zip(masks, pieces):
        slots = piece.shape[1]
        base = lax.bitwise_xor(me, mask) * slots
        for j in range(slots):
            row = jnp.where(base + j < count_ref[0], rows_ref[0, base + j], spare)
            product = jnp.dot(blocks_ref[cols_ref[0, base + j]], piece[0, j], preferred_element_type=jnp.float32)
            acc_ref[row] += product


def first_tiles(masks, rows_ref, cols_ref, count_ref, offsets_ref, blocks_ref, *refs):
    pieces, acc_ref = refs[:-1], refs[-1]
    for b in range(acc_ref.shape[0] - 1):
        acc_ref[b] = jnp.broadcast_to(offsets_ref[:, b * BLOCK : (b + 1) * BLOCK], acc_ref.shape[1:])
    acc_ref[acc_ref.shape[0] - 1] = jnp.zeros(acc_ref.shape[1:], jnp.float32)
    add_tiles(masks, blocks_ref, rows_ref, cols_ref, count_ref, pieces, acc_ref)


def last_tiles(masks, rows_ref, cols_ref, count_ref, quad_ref, blocks_ref, part_ref, *refs):
    pieces, (acc_ref, stats_ref) = refs[:-2], refs[-2:]
    for b in range(acc_ref.shape[0]):
        acc_ref[b] = part_ref[b]
    add_tiles(masks, blocks_ref, rows_ref, cols_ref, count_ref, pieces, acc_ref)
    cblocks = acc_ref.shape[0] - 1
    peak = acc_ref[0]
    for b in range(1, cblocks):
        peak = jnp.maximum(peak, acc_ref[b])
    peak = jnp.max(peak, axis=1, keepdims=True)
    mass = jnp.zeros(stats_ref.shape, jnp.float32)
    for b in range(cblocks):
        mass += jnp.exp(acc_ref[b] - peak)
    mass = jnp.sum(mass, axis=1, keepdims=True)
    lane = lax.broadcasted_iota(jnp.int32, stats_ref.shape, 1)
    stats_ref[...] = jnp.where(lane == 0, peak, jnp.where(lane == 1, mass, quad_ref[...]))


def merge(n_comp, fblocks, *refs):
    stats_refs, (inner_ref, own_ref, sum_ref) = refs[:-3], refs[-3:]
    here = lax.axis_index("comp")
    stats = [ref[...] for ref in stats_refs]
    if len(stats) == 2:
        swap = here == 1
        stats = [jnp.where(swap, stats[1], stats[0]), jnp.where(swap, stats[0], stats[1])]
    peaks = [part[:, 0:1] for part in stats]
    peak = functools.reduce(jnp.maximum, peaks)
    mass = functools.reduce(jnp.add, [part[:, 1:2] * jnp.exp(part[:, 0:1] - peak) for part in stats])
    quad = functools.reduce(jnp.add, [part[:, 2:3] for part in stats])
    inner = peak + jnp.log(mass)
    inner_ref[...] = jnp.broadcast_to(inner, inner_ref.shape)
    loglik = jnp.broadcast_to((quad + inner) / fblocks, inner_ref.shape)
    turned = jnp.transpose(loglik)
    share = own_ref.shape[1]
    npoints = inner_ref.shape[0]
    own_ref[...] = pltpu.roll(turned[0:8], lax.rem(n_comp - here, n_comp) * share, 1)[0:1, :share]
    sum_ref[...] = jnp.broadcast_to(jnp.sum(turned[0:8], axis=1, keepdims=True), sum_ref.shape)
    del npoints


def finish(acc_ref, inner_ref, out_ref):
    inner = inner_ref[...]
    for b in range(acc_ref.shape[0] - 1):
        out_ref[:, b * BLOCK : (b + 1) * BLOCK] = acc_ref[b] - inner


def on_device(data, base_precision, offsets, tile_values, tile_rows, tile_cols, tile_counts):
    n_pts, n_comp = lax.axis_size("pts"), lax.axis_size("comp")
    npoints, own_feats = data.shape
    fblocks = own_feats * n_comp // BLOCK
    cblocks = offsets.shape[0] // BLOCK
    bits = n_pts.bit_length() - 1
    low = 1 << (bits // 2)
    high = n_pts // low

    def flip(value, mask):
        return lax.ppermute(value, "pts", [(p, p ^ mask) for p in range(n_pts)])

    shifted = [
        lax.ppermute(data, "comp", [(c, (c + shift) % n_comp) for c in range(n_comp)]) for shift in range(1, n_comp)
    ]
    held = {0: tile_values}
    for k in sorted(range(1, high), reverse=True):
        held[k * low] = flip(tile_values, k * low)
    order = sorted(held)
    groups = [order[:2], order[2:]]
    pieces = {}
    for group in groups:
        for mask in group:
            pieces[mask] = held[mask]
        for m in range(1, low):
            for mask in group:
                pieces[mask ^ m] = flip(held[mask], m)
    masks = [[mask ^ m for mask in group for m in range(low)] for group in groups]

    f32 = jnp.float32
    square = jax.ShapeDtypeStruct((npoints, BLOCK), f32)
    blocks, quad = call(
        functools.partial(prepare, n_comp),
        "prepare",
        (jax.ShapeDtypeStruct((fblocks, npoints, BLOCK), data.dtype), square),
        [vmem] * (1 + n_comp),
        (base_precision[None, :], data, *shifted),
        10 * data.size,
    )
    acc_shape = jax.ShapeDtypeStruct((cblocks + 1, npoints, BLOCK), f32)
    tables = (tile_rows, tile_cols, tile_counts)
    per_tile = 2 * npoints * BLOCK * BLOCK
    acc = call(
        functools.partial(first_tiles, masks[0]),
        "first_tiles",
        acc_shape,
        [smem] * 3 + [vmem] * (2 + len(masks[0])),
        (*tables, offsets[None, :], blocks, *(pieces[mask] for mask in masks[0])),
        per_tile * len(masks[0]) * tile_values.shape[1],
    )
    acc, stats = call(
        functools.partial(last_tiles, masks[1]),
        "last_tiles",
        (acc_shape, square),
        [smem] * 3 + [vmem] * (3 + len(masks[1])),
        (*tables, quad, blocks, acc, *(pieces[mask] for mask in masks[1])),
        per_tile * len(masks[1]) * tile_values.shape[1],
    )
    if n_comp == 2:
        all_stats = [stats, lax.ppermute(stats, "comp", [(0, 1), (1, 0)])]
    else:
        gathered = lax.all_gather(stats, "comp")
        all_stats = [gathered[c] for c in range(n_comp)]
    share = npoints // n_comp
    inner, own, summed = call(
        functools.partial(merge, n_comp, fblocks),
        "merge",
        (square, jax.ShapeDtypeStruct((1, share), f32), jax.ShapeDtypeStruct((8, BLOCK), f32)),
        [vmem] * n_comp,
        all_stats,
        100 * npoints * BLOCK,
    )
    log_resp = call(
        finish,
        "finish",
        jax.ShapeDtypeStruct((npoints, cblocks * BLOCK), f32),
        [vmem] * 2,
        (acc, inner),
        npoints * cblocks * BLOCK,
    )
    for bit in range(bits):
        summed = summed + flip(summed, 1 << bit)
    mean_loglik = summed[0, 0] / (npoints * n_pts)
    return (log_resp, own.reshape(share), mean_loglik)


def solution(mesh):
    in_specs = (
        P("pts", "comp"),
        P("comp"),
        P("comp"),
        P("comp", "pts", None, None),
        P("comp", None),
        P("comp", None),
        P("comp"),
    )
    out_specs = (P("pts", "comp"), P(("pts", "comp")), P())
    return jax.shard_map(
        on_device, mesh=mesh, in_specs=in_specs, out_specs=out_specs, check_vma=False
    )
```
